32 devices in a mesh: row: 4 (over z), col: 8 (over y, x, core).
Axes of the slice: x: 2, y: 2, z: 4, core: 2. Of those that a mesh axis runs over, the one named last changes fastest.
Arguments:
- velocity: float32 [3, 64, 64, 256], P(None, 'row', 'col'), may hold values from -6 to 6
- positions: bfloat16 [1024, 3, 128], P(('row', 'col')), may hold values from -4 to 4
- weights: bfloat16 [1024, 3, 8, 128], P(('row', 'col')), may hold values from 0 to 0.5
- stiffness: bfloat16 [1024], P(('row', 'col')), may hold values from 0.099609375 to 1
- rest_sq: bfloat16 [1024], P(('row', 'col')), may hold values from 1 to 8
- owner_column: int32 [1024, 1], P(('row', 'col')), may hold values from 0 to 7; in each aligned block of 32 rows (0 to 31, 32 to 63, ...) at most 12 rows name the same one
- brick_index: int32 [1024], P(('row', 'col')), may hold values from 0 to 63
Outputs:
- new_velocity: float32 [3, 64, 64, 256], P(None, 'row', 'col')
- marker_velocity: float32 [1024, 3, 128], P(('row', 'col'))
The draws below stay inside these ranges and needn't reach their ends.
Inputs may be any that keep to these rules, and one draw needn't show every extreme that they name: `owner_column`: A block's brick lies on the device in the block's own device row and in this column; no device's 32 blocks name one column more than 12 times, and that many is reached.
All inputs are finite; a program needn't handle non-finite values.
Results may differ from the reference program's by a relative error of at most 0.0003.
Values may be sent and summed in bfloat16 or wider, within the bound.
A program may use at most 64 MiB of HBM per device.

```python
import math
import jax
import jax.numpy as jnp
import numpy as np
from jax import lax

CX = 16
CY = 8
NZ = 256
BRICK = 8
MARK = 128
BLK_DEV = 32
NX = 64
NY = 64
BLOCKS = 1024
CAP = 12
BRK_DEV = 64
N_ROW = 4
N_COL = 8


def set_ends(array, rng, smallest, high):
    place = [jax.random.randint(jax.random.fold_in(rng, axis), (), 0, length) for axis, length in enumerate(array.shape)]
    longest = array.shape.index(max(array.shape))
    beside = place[:longest] + [(place[longest] + 1) % array.shape[longest]] + place[longest + 1:]
    return array.at[tuple(place)].set(smallest).at[tuple(beside)].set(high)


def levels(key, dims, pieces, least, top_value):
    level, own = 1.0, jax.random.fold_in(key, 6)
    for axis_at, parts in pieces:
        heights = jnp.exp(jax.random.uniform(jax.random.fold_in(own, axis_at), (parts,), jnp.float32, least / len(pieces), top_value / len(pieces)))
        level = level * jnp.repeat(heights, dims[axis_at] // parts).reshape([-1 if axis == axis_at else 1 for axis in range(len(dims))])
    return level


def deal_out(stream_key, own, number, rows, amount, top, most, skew):
    sequence = jax.random.permutation(stream_key, amount)
    crowded, usual = load_shares(amount, rows * top, most, skew, True), load_shares(amount, rows * top, most, skew, False)
    places = jnp.arange(amount)

    def named(lengths, rotation):
        used = int((lengths > 0).sum())
        fixed = max(1, used // 4)
        moved = fixed + (places - fixed + rotation * (used - fixed)) % max(1, amount - fixed)
        return jnp.zeros((amount,), jnp.int32).at[sequence[jnp.where(places < fixed, places, moved)]].set(jnp.asarray(lengths, jnp.int32))

    lengths = jnp.where(number % 4 == 0, named(crowded, number // 4), named(usual, number - number // 4 - 1))
    mixed = jax.random.permutation(jax.random.fold_in(own, 3), amount)
    giver, sink = mixed[0:amount // 2 * 2:2], mixed[1:amount // 2 * 2:2]
    room = jnp.minimum(lengths[giver] - 1, most - lengths[sink]) // 2
    room = jnp.where((giver == sequence[0]) | (sink == sequence[0]) | (lengths[sink] == 0), 0, jnp.maximum(room, 0))
    moved = jax.random.randint(jax.random.fold_in(own, 4), (amount // 2,), 0, 1 << 20) % (room + 1)
    lengths = lengths.at[giver].add(-moved).at[sink].add(moved)
    labels = jnp.searchsorted(jnp.cumsum(lengths), jnp.arange(rows * top), side="right").astype(jnp.int32)
    table = labels.reshape(top, rows).T
    table = table[jax.random.permutation(jax.random.fold_in(own, 1), rows)]
    rotation = jax.random.randint(jax.random.fold_in(own, 2), (rows, 1), 0, top)
    return jnp.take_along_axis(table, (jnp.arange(top)[None, :] + rotation) % top, axis=1)


def load_shares(count, total, limit, lean, full):
    loads = [(1 << 20) // math.isqrt(grade ** lean) + 1 for grade in range(1, count + 1)]
    largest = limit if full else min(limit, max(-(-total // count), total * loads[0] // sum(loads)))
    least = 1 if total - largest >= count - 1 else 0
    counts, spare = [largest] + [least] * (count - 1), total - largest - least * (count - 1)
    while spare > 0:
        movable = [i for i in range(1, count) if counts[i] < largest] or [i for i in range(1, count) if counts[i] < limit]
        mass, budget = sum([loads[i] for i in movable]), spare
        for i in movable:
            addition = min(limit - counts[i], max(1, budget * loads[i] // mass), spare)
            counts[i] = counts[i] + addition
            spare = spare - addition
    return np.array(counts)


def normal_values(rng, extent, scale, most, pieces=(), held_as=jnp.bfloat16):
    factor_of = levels(rng, extent, pieces, -0.22, 0.18) if pieces else 1.0
    drawn = jax.random.normal(rng, extent, jnp.float32) * scale * factor_of
    return jnp.minimum(jnp.maximum(drawn, -most), most).astype(held_as)


def setup_inputs(seed: int = 0) -> dict:
    seeds = jax.random.split(jax.random.key(seed), 8)
    velocity = normal_values(seeds[0], (3, NX, NY, NZ), 1.0, 6.0, ((1, 4), (2, 8)), jnp.float32)
    positions = normal_values(seeds[1], (BLOCKS, 3, MARK), 1.0, 4.0, ((0, 32),))
    weights = jnp.clip(0.5 * jax.random.uniform(seeds[2], (BLOCKS, 3, BRICK, MARK), jnp.float32) ** levels(seeds[2], (BLOCKS, 3, BRICK, MARK), ((0, 32),), -0.2, 0.2), 0.0, 0.5).astype(jnp.bfloat16)
    stiffness = jnp.clip(jnp.exp(math.log(1.0) - 2.306499 * jax.random.uniform(seeds[3], (BLOCKS,), jnp.float32) ** levels(seeds[3], (BLOCKS,), ((0, 32),), -0.2, 0.2)), 0.099609375, 1.0).astype(jnp.bfloat16)
    rest_sq = jnp.clip(jnp.exp(math.log(8.0) - 2.0794415 * jax.random.uniform(seeds[4], (BLOCKS,), jnp.float32) ** levels(seeds[4], (BLOCKS,), ((0, 32),), -0.2, 0.2)), 1.0, 8.0).astype(jnp.bfloat16)
    owner_column_keys = jax.random.split(jax.random.fold_in(seeds[5], 1), BLOCKS // BLK_DEV)
    owner_column_turns = jax.random.permutation(jax.random.fold_in(seeds[5], 3), BLOCKS // BLK_DEV)
    owner_column = jax.vmap(lambda own, number: deal_out(jax.random.fold_in(seeds[5], 2), own, number, BLK_DEV, N_COL, 1, CAP, 2))(owner_column_keys, owner_column_turns).reshape((BLOCKS, 1))
    brick_index = set_ends(jax.random.randint(seeds[6], (BLOCKS,), 0, BRK_DEV), jax.random.fold_in(seeds[6], 1), 0, BRK_DEV - 1).astype(jnp.int32)
    return dict(velocity=velocity, positions=positions, weights=weights, stiffness=stiffness, rest_sq=rest_sq, owner_column=owner_column, brick_index=brick_index)


DT_STEP = 0.5
VISCOSITY = 0.1
PRECISE = lax.Precision.HIGHEST


def to_bricks(values):
    components, size_x, size_y, size_z = values.shape
    blocks_view = values.reshape(components, size_x // BRICK, BRICK, size_y // BRICK, BRICK, size_z // BRICK, BRICK)
    blocks_view = blocks_view.transpose(1, 3, 5, 0, 2, 4, 6)
    return blocks_view.reshape(-1, components * BRICK * BRICK * BRICK)


def from_bricks(bricks, size_x, size_y, size_z):
    blocks_view = bricks.reshape(size_x // BRICK, size_y // BRICK, size_z // BRICK, 3, BRICK, BRICK, BRICK)
    blocks_view = blocks_view.transpose(3, 0, 4, 1, 5, 2, 6)
    return blocks_view.reshape(3, size_x, size_y, size_z)


def chain_force(positions_f, stiffness_f, rest_f):
    segment = jnp.roll(positions_f, -1, axis=2) - positions_f
    stretch = jnp.sum(segment * segment, axis=1, keepdims=True) / rest_f[:, None, None]
    tension = 0.5 * stiffness_f[:, None, None] * (stretch - 1.0) * segment
    return tension - jnp.roll(tension, 1, axis=2)


def interpolate(bricks_in, weights_f):
    cubes = bricks_in.reshape(-1, 3, BRICK, BRICK, BRICK)
    reduced = jnp.einsum('ncijk,nkm->ncijm', cubes, weights_f[:, 2], precision=PRECISE)
    reduced = jnp.einsum('ncijm,njm->ncim', reduced, weights_f[:, 1], precision=PRECISE)
    return jnp.einsum('ncim,nim->ncm', reduced, weights_f[:, 0], precision=PRECISE)


def spread(forces, weights_f):
    partial_sum = jnp.einsum('ncm,nim->ncim', forces, weights_f[:, 0], precision=PRECISE)
    partial_sum = jnp.einsum('ncim,njm->ncijm', partial_sum, weights_f[:, 1], precision=PRECISE)
    cubes = jnp.einsum('ncijm,nkm->ncijk', partial_sum, weights_f[:, 2], precision=PRECISE)
    return cubes.reshape(cubes.shape[0], -1)


def advect(values):
    transport = jnp.zeros_like(values)
    for direction in range(3):
        gradient = (jnp.roll(values, -1, axis=direction + 1) - jnp.roll(values, 1, axis=direction + 1)) * 0.5
        transport = transport + values[direction] * gradient
    return transport


def signed_modes(indices, length):
    return jnp.where(indices <= (length - 1) // 2, indices, indices - length)


def direction_modes(indices, length):
    return jnp.where(2 * indices == length, 0, signed_modes(indices, length))


def reference(velocity, positions, weights, stiffness, rest_sq, owner_column, brick_index):
    brick_table = to_bricks(velocity)
    local_x = CX // BRICK
    local_y = CY // BRICK
    local_z = NZ // BRICK
    total_y = NY // BRICK
    block_ids = jnp.arange(BLOCKS, dtype=jnp.int32)
    row_index = block_ids // (BLK_DEV * N_COL)
    column = owner_column[:, 0]
    brick_x = brick_index // (local_y * local_z)
    brick_y = (brick_index // local_z) % local_y
    brick_z = brick_index % local_z
    global_ids = ((row_index * local_x + brick_x) * total_y + column * local_y + brick_y) * local_z + brick_z
    device_count = N_ROW * N_COL

    def visit_group(forcing, member):
        brick_ids, positions_g, weights_g, stiffness_g, rest_g = member
        weights_f = weights_g.astype(jnp.float32)
        marker_vel = interpolate(brick_table[brick_ids], weights_f)
        forces = chain_force(positions_g.astype(jnp.float32), stiffness_g.astype(jnp.float32), rest_g.astype(jnp.float32))
        forcing = forcing.at[brick_ids].add(spread(forces, weights_f))
        return forcing, marker_vel

    members = (global_ids.reshape(device_count, BLK_DEV),
               positions.reshape(device_count, BLK_DEV, 3, MARK),
               weights.reshape(device_count, BLK_DEV, 3, BRICK, MARK),
               stiffness.reshape(device_count, BLK_DEV),
               rest_sq.reshape(device_count, BLK_DEV))
    forcing, gathered = lax.scan(visit_group, jnp.zeros_like(brick_table), members)
    marker_velocity = gathered.reshape(BLOCKS, 3, MARK)
    force_field = from_bricks(forcing, NX, NY, NZ)
    star = velocity + DT_STEP * (force_field - advect(velocity))
    spectrum = jnp.fft.fftn(star, axes=(1, 2, 3))
    index_x = jnp.arange(NX, dtype=jnp.int32)
    index_y = jnp.arange(NY, dtype=jnp.int32)
    index_z = jnp.arange(NZ, dtype=jnp.int32)
    full_x = (2.0 * jnp.pi / NX) * signed_modes(index_x, NX).astype(jnp.float32)[:, None, None]
    full_y = (2.0 * jnp.pi / NY) * signed_modes(index_y, NY).astype(jnp.float32)[None, :, None]
    full_z = (2.0 * jnp.pi / NZ) * signed_modes(index_z, NZ).astype(jnp.float32)[None, None, :]
    dir_x = direction_modes(index_x, NX)[:, None, None]
    dir_y = direction_modes(index_y, NY)[None, :, None]
    dir_z = direction_modes(index_z, NZ)[None, None, :]
    no_direction = (dir_x == 0) & (dir_y == 0) & (dir_z == 0)
    wave_x = (2.0 * jnp.pi / NX) * dir_x.astype(jnp.float32)
    wave_y = (2.0 * jnp.pi / NY) * dir_y.astype(jnp.float32)
    wave_z = (2.0 * jnp.pi / NZ) * dir_z.astype(jnp.float32)
    wave_sq = wave_x * wave_x + wave_y * wave_y + wave_z * wave_z
    inverse_sq = jnp.where(no_direction, 0.0, 1.0 / jnp.where(no_direction, 1.0, wave_sq))
    damping = 1.0 / (1.0 + DT_STEP * VISCOSITY * (full_x * full_x + full_y * full_y + full_z * full_z))
    normal_part = (wave_x * spectrum[0] + wave_y * spectrum[1] + wave_z * spectrum[2]) * inverse_sq
    projected = jnp.stack([(spectrum[0] - wave_x * normal_part) * damping,
                           (spectrum[1] - wave_y * normal_part) * damping,
                           (spectrum[2] - wave_z * normal_part) * damping])
    new_velocity = jnp.real(jnp.fft.ifftn(projected, axes=(1, 2, 3))).astype(jnp.float32)
    return new_velocity, marker_velocity
```

```python
from functools import partial

import numpy as np

import jax
import jax.numpy as jnp
from jax import lax
from jax.experimental import pallas as pl
from jax.experimental.pallas import tpu as pltpu
from jax.sharding import PartitionSpec as P

BRICK = 8


DT_STEP = 0.5
VISCOSITY = 0.1
PRECISE = lax.Precision.HIGHEST


def with_halo(block, sides, width):
    for axis, dim in sides:
        count = lax.axis_size(axis)
        forward = [(i, i + 1) for i in range(count - 1)]
        forward.append((count - 1, 0))
        backward = [(target, source) for source, target in forward]
        low = lax.ppermute(
            lax.slice_in_dim(block, block.shape[dim] - width, None, axis=dim), axis, forward
        )
        high = lax.ppermute(lax.slice_in_dim(block, 0, width, axis=dim), axis, backward)
        block = jnp.concatenate([low, block, high], axis=dim)
    return block


def to_bricks(values):
    components, size_x, size_y, size_z = values.shape
    blocks_view = values.reshape(
        components, size_x // BRICK, BRICK, size_y // BRICK, BRICK, size_z // BRICK, BRICK
    )
    blocks_view = blocks_view.transpose(1, 3, 5, 0, 2, 4, 6)
    return blocks_view.reshape(-1, components * BRICK * BRICK * BRICK)


def from_bricks(bricks, size_x, size_y, size_z):
    blocks_view = bricks.reshape(
        size_x // BRICK, size_y // BRICK, size_z // BRICK, 3, BRICK, BRICK, BRICK
    )
    blocks_view = blocks_view.transpose(3, 0, 4, 1, 5, 2, 6)
    return blocks_view.reshape(3, size_x, size_y, size_z)


def chain_force(positions_f, stiffness_f, rest_f):
    segment = jnp.roll(positions_f, -1, axis=2) - positions_f
    stretch = jnp.sum(segment * segment, axis=1, keepdims=True) / rest_f[:, None, None]
    tension = 0.5 * stiffness_f[:, None, None] * (stretch - 1.0) * segment
    return tension - jnp.roll(tension, 1, axis=2)


def interpolate(bricks_in, weights_f):
    cubes = bricks_in.reshape(-1, 3, BRICK, BRICK, BRICK)
    reduced = jnp.einsum("ncijk,nkm->ncijm", cubes, weights_f[:, 2], precision=PRECISE)
    reduced = jnp.einsum("ncijm,njm->ncim", reduced, weights_f[:, 1], precision=PRECISE)
    return jnp.einsum("ncim,nim->ncm", reduced, weights_f[:, 0], precision=PRECISE)


def spread(forces, weights_f):
    partial_sum = jnp.einsum("ncm,nim->ncim", forces, weights_f[:, 0], precision=PRECISE)
    partial_sum = jnp.einsum("ncim,njm->ncijm", partial_sum, weights_f[:, 1], precision=PRECISE)
    cubes = jnp.einsum("ncijm,nkm->ncijk", partial_sum, weights_f[:, 2], precision=PRECISE)
    return cubes.reshape(cubes.shape[0], -1)


def signed_modes(indices, length):
    return jnp.where(indices <= (length - 1) // 2, indices, indices - length)


def direction_modes(indices, length):
    return jnp.where(2 * indices == length, 0, signed_modes(indices, length))


def tables(length):
    indices = jnp.arange(length, dtype=jnp.int32)
    phases = indices[:, None] * indices[None, :] % length
    angles = 2.0 * jnp.pi / length * phases.astype(jnp.float32)
    return (jnp.cos(angles), jnp.sin(angles))


def forward(form, real_part, imag_part, length):
    cosine, sine = tables(length)
    product = partial(jnp.einsum, precision=PRECISE)
    out_real = product(form, real_part, cosine) + product(form, imag_part, sine)
    out_imag = product(form, imag_part, cosine) - product(form, real_part, sine)
    return (out_real, out_imag)


def backward(form, real_part, imag_part, length):
    cosine, sine = tables(length)
    product = partial(jnp.einsum, precision=PRECISE)
    out_real = product(form, real_part, cosine) - product(form, imag_part, sine)
    out_imag = product(form, imag_part, cosine) + product(form, real_part, sine)
    return (out_real / length, out_imag / length)


def col_transpose(values):
    return lax.all_to_all(values, "col", split_axis=4, concat_axis=3, tiled=True)


def row_transpose(values):
    return lax.all_to_all(values, "row", split_axis=4, concat_axis=2, tiled=True)


def wave_parts(indices, length):
    scale = 2.0 * jnp.pi / length
    direct = direction_modes(indices, length)
    signed = signed_modes(indices, length)
    return (scale * direct.astype(jnp.float32), scale * signed.astype(jnp.float32), direct == 0)


def general(velocity, positions, weights, stiffness, rest_sq, owner_column, brick_index):
    row_count = lax.axis_size("row")
    col_count = lax.axis_size("col")
    size_x = velocity.shape[1]
    size_y = velocity.shape[2]
    size_z = velocity.shape[3]
    block_count = positions.shape[0]
    capacity = max(2, 3 * block_count // col_count)
    total_slots = col_count * capacity
    owner_col = owner_column[:, 0]
    order_ids = jnp.arange(block_count, dtype=jnp.int32)
    earlier_same = (owner_col[None, :] == owner_col[:, None]) & (
        order_ids[None, :] < order_ids[:, None]
    )
    slot_index = owner_col * capacity + jnp.sum(earlier_same.astype(jnp.int32), axis=1)
    stored = to_bricks(velocity)
    brick_count = stored.shape[0]

    def place(values, fill):
        buffer = jnp.full((total_slots,) + values.shape[1:], fill, values.dtype)
        return buffer.at[slot_index].set(values).reshape((col_count, capacity) + values.shape[1:])

    weights_f = weights.astype(jnp.float32)
    forces = chain_force(
        positions.astype(jnp.float32), stiffness.astype(jnp.float32), rest_sq.astype(jnp.float32)
    )
    pushed = spread(forces, weights_f)
    send_force = place(pushed, 0.0)
    send_index = place(brick_index.astype(jnp.float32), 0.0)
    wanted = lax.all_to_all(send_index, "col", split_axis=0, concat_axis=0, tiled=True)
    pushes = lax.all_to_all(send_force, "col", split_axis=0, concat_axis=0, tiled=True)
    wanted_ids = wanted.astype(jnp.int32)
    reply = stored[wanted_ids]
    returned = lax.all_to_all(reply, "col", split_axis=0, concat_axis=0, tiled=True)
    returned, arrived_ids, arrived = (returned, wanted_ids, pushes)
    fetched = returned.reshape(total_slots, -1)[slot_index]
    marker_velocity = interpolate(fetched, weights_f)
    forcing = jax.ops.segment_sum(
        arrived.reshape(total_slots, -1), arrived_ids.reshape(-1), num_segments=brick_count
    )
    force_field = from_bricks(forcing, size_x, size_y, size_z)
    padded = with_halo(velocity, (("row", 1), ("col", 2)), 1)
    grad_x = (padded[:, 2:, 1:-1] - padded[:, :-2, 1:-1]) * 0.5
    grad_y = (padded[:, 1:-1, 2:] - padded[:, 1:-1, :-2]) * 0.5
    grad_z = (jnp.roll(velocity, -1, axis=3) - jnp.roll(velocity, 1, axis=3)) * 0.5
    transport = velocity[0] * grad_x + velocity[1] * grad_y + velocity[2] * grad_z
    star = velocity + DT_STEP * (force_field - transport)
    cos_z, sin_z = tables(size_z)
    half_z = size_z // 2
    col_here = lax.axis_index("col")
    cos_fore = cos_z[:, :half_z]
    sin_fore = sin_z[:, :half_z].at[:, 0].set(-cos_z[:, half_z])
    z_real = jnp.einsum("cxyz,zk->cxyk", star, cos_fore, precision=PRECISE)
    z_imag = -jnp.einsum("cxyz,zk->cxyk", star, sin_fore, precision=PRECISE)
    shuffled = col_transpose(jnp.stack([z_real, z_imag]))
    slab = shuffled.shape[4]
    first_slot = (col_here == 0) & (jnp.arange(slab, dtype=jnp.int32) == 0)
    highest = shuffled[1][..., 0:1] * (col_here == 0).astype(jnp.float32)
    lower_imag = jnp.where(first_slot, 0.0, shuffled[1])
    y_in_real = jnp.concatenate([shuffled[0], highest], axis=3)
    y_in_imag = jnp.concatenate([lower_imag, jnp.zeros_like(highest)], axis=3)
    z_index = jnp.concatenate(
        [col_here * slab + jnp.arange(slab, dtype=jnp.int32), jnp.full((1,), half_z, jnp.int32)]
    )
    y_real, y_imag = forward("cxyz,yk->cxzk", y_in_real, y_in_imag, y_in_real.shape[2])
    shuffled = row_transpose(jnp.stack([y_real, y_imag]))
    x_real, x_imag = forward("cxzy,xk->czyk", shuffled[0], shuffled[1], shuffled.shape[2])
    slab_y = x_real.shape[2]
    full_x = x_real.shape[3]
    full_y = slab_y * row_count
    y_index = lax.axis_index("row") * slab_y + jnp.arange(slab_y, dtype=jnp.int32)
    x_index = jnp.arange(full_x, dtype=jnp.int32)
    dir_z, sig_z, zero_z = wave_parts(z_index, size_z)
    dir_y, sig_y, zero_y = wave_parts(y_index, full_y)
    dir_x, sig_x, zero_x = wave_parts(x_index, full_x)
    wave_z = dir_z[:, None, None]
    wave_y = dir_y[None, :, None]
    wave_x = dir_x[None, None, :]
    no_direction = zero_z[:, None, None] & zero_y[None, :, None] & zero_x[None, None, :]
    wave_sq = wave_x * wave_x + wave_y * wave_y + wave_z * wave_z
    full_sq = sig_z[:, None, None] ** 2 + sig_y[None, :, None] ** 2 + sig_x[None, None, :] ** 2
    inverse_sq = jnp.where(no_direction, 0.0, 1.0 / jnp.where(no_direction, 1.0, wave_sq))
    damping = 1.0 / (1.0 + DT_STEP * VISCOSITY * full_sq)
    waves = jnp.stack(
        [
            jnp.broadcast_to(wave_x, wave_sq.shape),
            jnp.broadcast_to(wave_y, wave_sq.shape),
            jnp.broadcast_to(wave_z, wave_sq.shape),
        ]
    )
    normal_real = jnp.sum(waves * x_real, axis=0) * inverse_sq
    normal_imag = jnp.sum(waves * x_imag, axis=0) * inverse_sq
    p_real = (x_real - waves * normal_real) * damping
    p_imag = (x_imag - waves * normal_imag) * damping
    b_real, b_imag = backward("czyk,kx->cyzx", p_real, p_imag, full_x)
    shuffled = row_transpose(jnp.stack([b_real, b_imag]))
    b_real, b_imag = backward("cyzx,yk->cxzk", shuffled[0], shuffled[1], shuffled.shape[2])
    slab = b_real.shape[2] - 1
    first_slot = (col_here == 0) & (jnp.arange(slab, dtype=jnp.int32) == 0)
    highest = b_real[:, :, slab:, :]
    packed_imag = jnp.where(first_slot[None, None, :, None], highest, b_imag[:, :, :slab, :])
    shuffled = col_transpose(jnp.stack([b_real[:, :, :slab, :], packed_imag]))
    doubling = jnp.where(jnp.arange(half_z, dtype=jnp.int32) == 0, 1.0, 2.0)[:, None]
    cos_back = cos_z[:half_z] * doubling
    sin_back = (sin_z[:half_z] * doubling).at[0].set(-cos_z[half_z])
    new_velocity = (
        jnp.einsum("cxky,kz->cxyz", shuffled[0], cos_back, precision=PRECISE)
        - jnp.einsum("cxky,kz->cxyz", shuffled[1], sin_back, precision=PRECISE)
    ) / size_z
    return (new_velocity, marker_velocity)


VMEM = pltpu.VMEM
SMEM = pltpu.SMEM
MESH = pl.DeviceIdType.MESH
F32 = jnp.float32
BF16 = jnp.bfloat16


def two_parts(table):
    table = np.asarray(table, np.float64)
    high = table.astype(jnp.bfloat16)
    low = (table - high.astype(np.float64)).astype(jnp.bfloat16)
    return np.stack([high, low])


def angle_of(length, left, right):
    return 2.0 * np.pi / length * (np.outer(left, right) % length)


def build_tables(size_x, size_y, size_z, devices, rows, local_x):
    half_z = size_z // 2
    modes = half_z // devices
    z = np.arange(size_z)
    fore = np.zeros((devices, 2, modes, size_z))
    back = np.zeros((devices, 2, modes, size_z))
    turn = angle_of(size_z, np.arange(half_z), z).reshape(devices, modes, size_z)
    fore[:, 0], fore[:, 1] = np.cos(turn), -np.sin(turn)
    back[:, 0], back[:, 1] = 2.0 * np.cos(turn), -2.0 * np.sin(turn)
    alternate = np.where(z % 2 == 0, 1.0, -1.0)
    fore[0, 1, 0] = alternate
    back[0, 0, 0], back[0, 1, 0] = 1.0, alternate
    back = back / (size_x * size_y * size_z)
    turn_y = angle_of(size_y, np.arange(size_y), np.arange(size_y))
    y_fore = np.concatenate([np.cos(turn_y), np.sin(turn_y)], axis=0)
    y_back = np.concatenate([np.cos(turn_y), np.sin(turn_y)], axis=1)
    turn_x = angle_of(size_x, np.arange(size_x), np.arange(size_x)).reshape(rows, local_x, size_x)
    cosine, sine = np.cos(turn_x), np.sin(turn_x)
    base = np.zeros((rows, 2, local_x, 2, modes, 2, size_x))
    base[:, 0, :, 0, :, 0] = cosine[:, :, None]
    base[:, 0, :, 0, :, 1] = -sine[:, :, None]
    base[:, 1, :, 1, :, 0] = cosine[:, :, None]
    base[:, 1, :, 1, :, 1] = -sine[:, :, None]
    base[:, 0, :, 1, :, 0] = sine[:, :, None]
    base[:, 0, :, 1, :, 1] = cosine[:, :, None]
    base[:, 1, :, 0, :, 0] = -sine[:, :, None]
    base[:, 1, :, 0, :, 1] = -cosine[:, :, None]
    top = np.zeros_like(base)
    top[:, :, :, 1, 0] = base[:, :, :, 0, 0]
    out = np.zeros_like(base)
    out[:, 0, :, 0, :, 0] = cosine[:, :, None]
    out[:, 0, :, 0, :, 1] = -sine[:, :, None]
    out[:, 0, :, 1, :, 0] = sine[:, :, None]
    out[:, 0, :, 1, :, 1] = cosine[:, :, None]
    out[:, 1, :, 0, :, 0] = -sine[:, :, None]
    out[:, 1, :, 0, :, 1] = -cosine[:, :, None]
    out[:, 1, :, 1, :, 0] = cosine[:, :, None]
    out[:, 1, :, 1, :, 1] = -sine[:, :, None]
    top_out = np.zeros_like(out)
    top_out[:, :, :, 1, 0] = out[:, :, :, 0, 0]
    wide = rows * 2 * local_x * 2 * modes
    square = (wide, 2 * size_x)
    return (
        two_parts(fore.reshape(-1, size_z)),
        two_parts(back.reshape(-1, size_z)),
        two_parts(y_fore),
        two_parts(y_back),
        two_parts(base.reshape(square)),
        two_parts(top.reshape(square)),
        two_parts(out.reshape(square).T),
        two_parts(top_out.reshape(square).T),
    )


def parts(values):
    high = values.astype(BF16)
    return high, (values - high.astype(F32)).astype(BF16)


def mul(left, right, dims=((1,), (0,))):
    return lax.dot_general(left, right, (dims, ((), ())), preferred_element_type=F32)


def mul3(left, right, dims=((1,), (0,))):
    return (
        mul(left[0], right[0], dims) + mul(left[1], right[0], dims) + mul(left[0], right[1], dims)
    )


def swap_tile(values):
    sub = lax.broadcasted_iota(jnp.int32, values.shape, 1)
    lane = lax.broadcasted_iota(jnp.int32, values.shape, 2)
    for bit in range(3):
        step = 1 << bit
        sub_bit = (sub >> bit) & 1
        lane_bit = (lane >> bit) & 1
        up = pltpu.roll(pltpu.roll(values, 8 - step, 1), step, 2)
        down = pltpu.roll(pltpu.roll(values, step, 1), 128 - step, 2)
        other = jnp.where(sub_bit == 0, up, down)
        values = jnp.where(sub_bit == lane_bit, values, other)
    return values


def spread_kernel(
    capacity, owner_ref, brick_ref, stiff_ref, rest_ref, pos_ref, weight_ref, velocity_ref,
    push_ref, slot_ref, face_x_ref, face_y_ref, buf, ids, count,
):
    columns = push_ref.shape[0]
    blocks = pos_ref.shape[0]
    rows = capacity * 8
    buf[...] = jnp.zeros_like(buf)
    ids[...] = jnp.full(ids.shape, -1.0, F32)
    for col in range(columns):
        count[col] = 0
    last_x = velocity_ref.shape[1] - 1
    face_x_ref[0] = velocity_ref[:, last_x]
    face_x_ref[1] = velocity_ref[:, 0]
    last_y = velocity_ref.shape[2] - 1
    face_y_ref[0] = velocity_ref[:, :, last_y, :]
    face_y_ref[1] = velocity_ref[:, :, 0, :]

    def block(index, carry):
        owner = owner_ref[index]
        rank = count[owner]
        count[owner] = rank + 1
        slot = owner * capacity + rank
        slot_ref[index] = slot
        lane = lax.broadcasted_iota(jnp.int32, (1, 128), 1)
        mark = (brick_ref[index] * 8 + (lane & 7)).astype(F32)
        ids[pl.ds(owner, 1), :] = jnp.where((lane >> 3) == rank, mark, ids[pl.ds(owner, 1), :])
        place = pos_ref[index].astype(F32)
        segment = pltpu.roll(place, 127, 1) - place
        stretch = jnp.sum(segment * segment, axis=0, keepdims=True) / rest_ref[index]
        tension = 0.5 * stiff_ref[index] * (stretch - 1.0) * segment
        force = tension - pltpu.roll(tension, 1, 1)
        first = weight_ref[index, 0].astype(F32)
        second = weight_ref[index, 1].astype(F32)
        third = weight_ref[index, 2]
        both = (first[:, None, :] * second[None, :, :]).reshape(64, 128)
        spreads = jnp.concatenate([force[c : c + 1] * both for c in range(3)], axis=0)
        high, low = parts(spreads)
        cube = mul(third, high, ((1,), (1,))) + mul(third, low, ((1,), (1,)))
        buf[pl.ds(pl.multiple_of(slot * 8, 8), 8), 0:192] = cube
        return carry

    lax.fori_loop(0, blocks, block, 0)
    half = rows // 2
    lane = lax.broadcasted_iota(jnp.int32, (half, 128), 1)
    for col in range(columns):
        start = col * rows
        push_ref[col, 0:rows] = buf[start : start + rows, 0:128]
        lower = buf[start : start + half, 128:256]
        upper = pltpu.roll(buf[start + half : start + rows, 128:256], 64, 1)
        push_ref[col, rows : rows + half] = jnp.where(lane < 64, lower, upper)
        push_ref[col, rows + half :] = jnp.broadcast_to(ids[col : col + 1, :], (8, 128))


def star_kernel(
    capacity, velocity_ref, face_x_ref, face_y_ref, push_ref, fore_ref,
    send_ref, reply_ref, select, gathered,
):
    columns = push_ref.shape[0]
    rows = capacity * 8
    half = rows // 2
    size_x, size_y, size_z = velocity_ref.shape[1:]
    bricks_x = size_x // 8
    gathered[...] = jnp.zeros_like(gathered)
    line = lax.broadcasted_iota(jnp.int32, (bricks_x * size_z, 128), 0).astype(F32)
    for col in range(columns):
        start = col * 128
        gathered[start : start + rows, 0:128] = push_ref[col, 0:rows]
        rest = push_ref[col, rows : rows + half]
        gathered[start : start + half, 128:256] = rest
        gathered[start + half : start + rows, 128:256] = pltpu.roll(rest, 64, 1)
        mark = push_ref[col, rows + half : rows + half + 1, :]
        select[:, start : start + 128] = jnp.where(line == mark, 1.0, 0.0).astype(BF16)
    high, low = parts(gathered[...])
    field = []
    reply = None
    for brick in range(bricks_x):
        chosen = select[brick * size_z : (brick + 1) * size_z, :]
        turned = mul(chosen, high) + mul(chosen, low)
        force = turned.T[0:192].reshape(3, 8, 8, size_z)
        field.append(force)
        piece = velocity_ref[:, brick * 8 : (brick + 1) * 8].reshape(192, size_z)
        p_high, p_low = parts(piece)
        part = mul(p_high, chosen) + mul(p_low, chosen)
        reply = part if reply is None else reply + part
    lane = lax.broadcasted_iota(jnp.int32, (half, 128), 1)
    for col in range(columns):
        back = reply[:, col * 128 : (col + 1) * 128].T
        reply_ref[col, 0:rows] = back[0:rows, 0:128]
        side = jnp.concatenate([back[0:rows, 128:192], back[0:rows, 128:192]], axis=1)
        reply_ref[col, rows:] = jnp.where(lane < 64, side[0:half], side[half:rows])
    force = jnp.concatenate(field, axis=1)
    value = velocity_ref[...]
    ahead = jnp.concatenate([value[:, 1:], face_x_ref[1][:, None]], axis=1)
    behind = jnp.concatenate([face_x_ref[0][:, None], value[:, :-1]], axis=1)
    transport = value[0:1] * ((ahead - behind) * 0.5)
    flat = value.reshape(3 * size_x, size_y, size_z)
    sub = lax.broadcasted_iota(jnp.int32, flat.shape, 1)
    face_low = face_y_ref[0].reshape(3 * size_x, 1, size_z)
    face_high = face_y_ref[1].reshape(3 * size_x, 1, size_z)
    ahead = jnp.where(sub == size_y - 1, face_high, pltpu.roll(flat, size_y - 1, 1))
    behind = jnp.where(sub == 0, face_low, pltpu.roll(flat, 1, 1))
    transport += value[1:2] * ((ahead - behind) * 0.5).reshape(value.shape)
    ahead = pltpu.roll(flat, size_z - 1, 2)
    behind = pltpu.roll(flat, 1, 2)
    transport += value[2:3] * ((ahead - behind) * 0.5).reshape(value.shape)
    star = value + DT_STEP * (force - transport)
    star_parts = parts(star.reshape(3 * size_x * size_y, size_z))
    modes = mul3((fore_ref[0], fore_ref[1]), star_parts, ((1,), (1,)))
    for c in range(3):
        tile = modes[:, c * 128 : (c + 1) * 128].reshape(-1, 8, 128)
        send_ref[:, c] = swap_tile(tile)


def middle_kernel(
    rows, columns, size_z, here_ref, recv_ref, y_fore_ref, y_back_ref, base_ref, top_ref, out_ref,
    top_out_ref, send_ref, wide,
):
    size_y = y_back_ref.shape[1]
    size_x = base_ref.shape[2] // 2
    here = here_ref[0]
    first = here == 0
    y_fore = (y_fore_ref[0], y_fore_ref[1])
    y_back = (y_back_ref[0], y_back_ref[1])
    for r in range(rows):
        for c in range(3):
            plane = recv_ref[r * columns : (r + 1) * columns, c].reshape(size_y, 128)
            both = mul3(y_fore, parts(plane))
            wide[c * size_y : (c + 1) * size_y, r * 256 : r * 256 + 128] = both[0:size_y]
            wide[c * size_y : (c + 1) * size_y, r * 256 + 128 : r * 256 + 256] = both[size_y:]
    left = parts(wide[...])
    sub = lax.broadcasted_iota(jnp.int32, base_ref.shape[1:], 0)
    lane = lax.broadcasted_iota(jnp.int32, out_ref.shape[1:], 1)
    index = lax.broadcasted_iota(jnp.int32, (size_y, 2 * size_x), 1) & (size_x - 1)
    line = lax.broadcasted_iota(jnp.int32, (size_y, 2 * size_x), 0)
    scale_x, scale_y, scale_z = (2.0 * np.pi / n for n in (size_x, size_y, size_z))
    sig_x = jnp.where(index < size_x // 2, index, index - size_x).astype(F32) * scale_x
    sig_y = jnp.where(line < size_y // 2, line, line - size_y).astype(F32) * scale_y
    wave_x = jnp.where(index == size_x // 2, 0.0, sig_x)
    wave_y = jnp.where(line == size_y // 2, 0.0, sig_y)
    total = None
    for slot in range(5):
        if slot < 4:
            keep = (sub & 3) == slot
            spare = (lane & 3) == slot
            if slot == 0:
                keep = keep & jnp.logical_not(first & ((sub & 7) == 4))
                spare = spare & jnp.logical_not(first & ((lane & 7) == 4))
            matrix = [jnp.where(keep, base_ref[p].astype(F32), 0.0).astype(BF16) for p in range(2)]
            inverse = [jnp.where(spare, out_ref[p].astype(F32), 0.0).astype(BF16) for p in range(2)]
            mode = here * 4 + slot
            sig_z = mode.astype(F32) * scale_z
            wave_z = sig_z
        else:
            matrix = [top_ref[0], top_ref[1]]
            spare = first & (lane >= 0)
            inverse = [
                jnp.where(spare, top_out_ref[p].astype(F32), 0.0).astype(BF16) for p in range(2)
            ]
            sig_z = F32(np.pi)
            wave_z = F32(0.0)
        spectrum = mul3(left, matrix)
        x, y, z = (spectrum[c * size_y : (c + 1) * size_y] for c in range(3))
        square = wave_x * wave_x + wave_y * wave_y + wave_z * wave_z
        full = sig_x * sig_x + sig_y * sig_y + sig_z * sig_z
        none = square == 0.0
        inverse_sq = jnp.where(none, 0.0, 1.0 / jnp.where(none, 1.0, square))
        damping = 1.0 / (1.0 + DT_STEP * VISCOSITY * full)
        normal = (wave_x * x + wave_y * y + wave_z * z) * inverse_sq
        result = jnp.concatenate(
            [
                (x - wave_x * normal) * damping,
                (y - wave_y * normal) * damping,
                (z - wave_z * normal) * damping,
            ],
            axis=0,
        )
        piece = mul3(parts(result), inverse)
        total = piece if total is None else total + piece
    wide[...] = total
    for r in range(rows):
        for c in range(3):
            pair = jnp.concatenate(
                [
                    wide[c * size_y : (c + 1) * size_y, r * 256 : r * 256 + 128],
                    wide[c * size_y : (c + 1) * size_y, r * 256 + 128 : r * 256 + 256],
                ],
                axis=0,
            )
            plane = mul3(y_back, parts(pair))
            send_ref[r * columns : (r + 1) * columns, c] = plane.reshape(columns, 8, 128)


def final_kernel(recv_ref, back_ref, new_ref):
    turned = []
    for c in range(3):
        turned.append(swap_tile(recv_ref[:, c]).reshape(-1, 128))
    values = parts(jnp.concatenate(turned, axis=1).T)
    result = mul3(values, (back_ref[0], back_ref[1]))
    new_ref[...] = result.reshape(new_ref.shape)


def marker_kernel(capacity, slot_ref, reply_ref, weight_ref, out_ref, buf):
    columns = reply_ref.shape[0]
    blocks = weight_ref.shape[0]
    rows = capacity * 8
    half = rows // 2
    for col in range(columns):
        start = col * rows
        buf[start : start + rows, 0:128] = reply_ref[col, 0:rows]
        rest = reply_ref[col, rows : rows + half]
        buf[start : start + half, 128:256] = rest
        buf[start + half : start + rows, 128:256] = pltpu.roll(rest, 64, 1)

    def block(index, carry):
        slot = slot_ref[index]
        cube = buf[pl.ds(pl.multiple_of(slot * 8, 8), 8), :]
        high, low = parts(cube.T)
        third = weight_ref[index, 2]
        deep = (mul(high, third) + mul(low, third))[0:192].reshape(3, 8, 8, 128)
        first = weight_ref[index, 0].astype(F32)
        second = weight_ref[index, 1].astype(F32)
        summed = jnp.sum(deep * first[None, :, None, :], axis=1)
        out_ref[index] = jnp.sum(summed * second[None], axis=1)
        return carry

    lax.fori_loop(0, blocks, block, 0)


def exchange(items, ident):
    groups = sorted({axes for _, axes in items if axes != "ring"}, key=len)
    sizes = []
    for array, axes in items:
        sizes.append(array.shape[0])

    def kernel(*refs):
        count = len(items)
        sources, targets, sems = refs[:count], refs[count : 2 * count], refs[2 * count :]
        row, col = lax.axis_index("row"), lax.axis_index("col")
        rows, cols = lax.axis_size("row"), lax.axis_size("col")
        barrier = pltpu.get_barrier_semaphore()

        def peer(axes, step):
            if axes == ("row", "col"):
                at = lax.rem(row * cols + col + step, rows * cols)
                return (at // cols, lax.rem(at, cols)), at
            if axes == ("col",):
                at = lax.rem(col + step, cols)
                return (row, at), at
            at = lax.rem(row + step, rows)
            return (at, col), at

        greet = []
        if any(axes == ("row", "col") for _, axes in items):
            greet = [(("row", "col"), step) for step in range(1, rows * cols)]
        else:
            greet = [(("col",), step) for step in range(1, cols)]
            greet += [(("row",), step) for step in sorted({1, rows - 1})]
        for axes, step in greet:
            device, _ = peer(axes, step)
            pl.semaphore_signal(barrier, inc=1, device_id=device, device_id_type=MESH)
        pl.semaphore_wait(barrier, len(greet))
        waits = []
        for number, (_, axes) in enumerate(items):
            source, target = sources[number], targets[number]
            send, receive = sems[2 * number], sems[2 * number + 1]
            if axes[0] == "near":
                along = (axes[1],)
                extent = rows if axes[1] == "row" else cols
                for side, step in ((0, 1), (1, extent - 1)):
                    device, _ = peer(along, step)
                    copy = pltpu.make_async_remote_copy(
                        source.at[side], target.at[side], send.at[side], receive.at[side],
                        device_id=device, device_id_type=MESH,
                    )
                    copy.start()
                    waits.append((copy, copy))
                continue
            extent = sizes[number]
            _, me = peer(axes, 0)
            for step in range(1, extent):
                device, at = peer(axes, step)
                copy = pltpu.make_async_remote_copy(
                    source.at[at], target.at[me], send.at[step], receive.at[step],
                    device_id=device, device_id_type=MESH,
                )
                copy.start()
                _, origin = peer(axes, extent - step)
                arrival = pltpu.make_async_remote_copy(
                    source.at[at], target.at[origin], send.at[step], receive.at[step],
                    device_id=device, device_id_type=MESH,
                )
                waits.append((copy, arrival))
            own = pltpu.make_async_copy(source.at[me], target.at[me], send.at[0])
            own.start()
            waits.append((own, None))
        for copy, arrival in waits:
            if arrival is None:
                copy.wait()
            else:
                copy.wait_send()
                arrival.wait_recv()

    scratch = []
    for array, _ in items:
        scratch += [pltpu.SemaphoreType.DMA((array.shape[0],))] * 2
    return pl.pallas_call(
        kernel,
        out_shape=[jax.ShapeDtypeStruct(a.shape, a.dtype) for a, _ in items],
        in_specs=[pl.BlockSpec(memory_space=VMEM)] * len(items),
        out_specs=[pl.BlockSpec(memory_space=VMEM)] * len(items),
        scratch_shapes=scratch,
        compiler_params=pltpu.CompilerParams(collective_id=ident, has_side_effects=True),
        name="exchange%d" % ident,
    )(*[a for a, _ in items])


def local(velocity, positions, weights, stiffness, rest_sq, owner_column, brick_index):
    rows = lax.axis_size("row")
    columns = lax.axis_size("col")
    devices = rows * columns
    _, local_x, local_y, size_z = velocity.shape
    blocks = positions.shape[0]
    capacity = max(2, 3 * blocks // columns)
    bricks = (local_x // BRICK) * (local_y // BRICK) * (size_z // BRICK)
    fits = (
        local_x == 16 and local_y == 8 and size_z == 8 * devices and positions.shape[2] == 128
        and capacity % 2 == 0 and capacity <= 16 and columns * local_y == 64
        and rows * local_x == 64 and bricks * BRICK == local_x // BRICK * size_z
    )
    if not fits:
        return general(
            velocity, positions, weights, stiffness, rest_sq, owner_column, brick_index
        )
    return fast(velocity, positions, weights, stiffness, rest_sq, owner_column, brick_index)


def fast(velocity, positions, weights, stiffness, rest_sq, owner_column, brick_index):
    rows = lax.axis_size("row")
    columns = lax.axis_size("col")
    devices = rows * columns
    _, local_x, local_y, size_z = velocity.shape
    blocks = positions.shape[0]
    capacity = max(2, 3 * blocks // columns)
    size_x, size_y = rows * local_x, columns * local_y
    fore, back, y_fore, y_back, base, top, out, top_out = build_tables(
        size_x, size_y, size_z, devices, rows, local_x
    )
    slots = capacity * 8
    length = slots + slots // 2
    vm = pl.BlockSpec(memory_space=VMEM)
    sm = pl.BlockSpec(memory_space=SMEM)
    shape = jax.ShapeDtypeStruct
    push, slot, face_x, face_y = pl.pallas_call(
        partial(spread_kernel, capacity),
        out_shape=[
            shape((columns, length + 8, 128), F32),
            shape((blocks,), jnp.int32),
            shape((2, 3, local_y, size_z), F32),
            shape((2, 3, local_x, size_z), F32),
        ],
        in_specs=[sm, sm, sm, sm, vm, vm, vm],
        out_specs=[vm, sm, vm, vm],
        scratch_shapes=[
            VMEM((columns * slots, 256), F32),
            VMEM((columns, 128), F32),
            SMEM((columns,), jnp.int32),
        ],
        name="spread",
    )(
        owner_column[:, 0], brick_index, stiffness.astype(F32), rest_sq.astype(F32), positions,
        weights, velocity,
    )
    push, face_x, face_y = exchange(
        [(push, ("col",)), (face_x, ("near", "row")), (face_y, ("near", "col"))], 1
    )
    send, reply = pl.pallas_call(
        partial(star_kernel, capacity),
        out_shape=[shape((devices, 3, 8, 128), F32), shape((columns, length, 128), F32)],
        in_specs=[vm] * 5,
        out_specs=[vm, vm],
        scratch_shapes=[
            VMEM((local_x // BRICK * size_z, columns * 128), BF16),
            VMEM((columns * 128, 256), F32),
        ],
        name="star",
    )(velocity, face_x, face_y, push, fore)
    send, reply = exchange([(send, ("row", "col")), (reply, ("col",))], 2)
    here = (lax.axis_index("row") * columns + lax.axis_index("col")).astype(jnp.int32)
    send = pl.pallas_call(
        partial(middle_kernel, rows, columns, size_z),
        out_shape=shape((devices, 3, 8, 128), F32),
        in_specs=[sm] + [vm] * 7,
        out_specs=vm,
        scratch_shapes=[VMEM((3 * size_y, rows * 256), F32)],
        name="middle",
    )(here.reshape(1), send, y_fore, y_back, base, top, out, top_out)
    (send,) = exchange([(send, ("row", "col"))], 3)
    marker_velocity = pl.pallas_call(
        partial(marker_kernel, capacity),
        out_shape=shape((blocks, 3, 128), F32),
        in_specs=[sm, vm, vm],
        out_specs=vm,
        scratch_shapes=[VMEM((columns * slots, 256), F32)],
        name="markers",
    )(slot, reply, weights)
    new_velocity = pl.pallas_call(
        final_kernel,
        out_shape=shape(velocity.shape, F32),
        in_specs=[vm, vm],
        out_specs=vm,
        name="final",
    )(send, back)
    return new_velocity, marker_velocity


def solution(mesh):
    return jax.shard_map(
        local,
        mesh=mesh,
        in_specs=(
            P(None, "row", "col", None),
            P(("row", "col"), None, None),
            P(("row", "col"), None, None, None),
            P(("row", "col")),
            P(("row", "col")),
            P(("row", "col"), None),
            P(("row", "col")),
        ),
        out_specs=(P(None, "row", "col", None), P(("row", "col"), None, None)),
        check_vma=False,
    )
```
